256 devices in a mesh: ctx: 32 (over x, z_hi, core), head: 8 (over z_lo, y).
Axes of the slice: x: 4, y: 4, z: 8 (z_hi: 4, z_lo: 2; z = z_hi * 2 + z_lo), core: 2. Of those that a mesh axis runs over, the one named last changes fastest.
Arguments:
- queries: bfloat16 [4096, 64, 576], P('ctx', 'head'), may hold values from -512 to 512
- latents: bfloat16 [4096, 576], P('ctx'), may hold values from -4 to 4
- index_queries: bfloat16 [4096, 64, 128], P('ctx', 'head'), may hold values from -512 to 512
- index_keys: bfloat16 [4096, 128], P('ctx'), may hold values from -4 to 4
- head_weights: float32 [4096, 64], P('ctx', 'head'), may hold values from -1.5 to 1.5
- block_pos: int32 [32], replicated, may hold values from 0 to 31, each once
Outputs:
- grad_index_queries: float32 [4096, 64, 128], P('ctx', 'head')
- grad_index_keys: float32 [4096, 128], P('ctx')
The draws below stay inside these ranges and needn't reach their ends.
All inputs are finite; a program needn't handle non-finite values.
Results may differ from the reference program's by a relative error of at most 0.008.
Values may be sent and summed in bfloat16 or wider, within the bound.
No kernel may reach another device: no remote copies, remote signals or barrier semaphores. Data moves between devices by JAX's collectives and lax.ppermute only.
A program may use at most 128 MiB of HBM per device.

```python
import jax
import jax.numpy as jnp
from jax import lax

HEADS = 64
RANK = 576
IHEADS = 64
IDIM = 128
TOK_DEV = 128
SEQ = 4096
BLOCKS = 32


def context_draw(key):
    pieces = jax.random.split(jax.random.fold_in(key, 7), 5)
    latent = jnp.clip(jax.random.normal(pieces[0], (SEQ, RANK), jnp.float32), -4.0, 4.0)
    latent = latent.astype(jnp.bfloat16).astype(jnp.float32)
    ikeys = jnp.clip(jax.random.normal(pieces[1], (SEQ, IDIM), jnp.float32), -4.0, 4.0)
    ikeys = ikeys.astype(jnp.bfloat16).astype(jnp.float32)
    weights = jnp.clip(0.3 * jax.random.normal(pieces[2], (SEQ, IHEADS), jnp.float32), -1.5, 1.5)
    query = jnp.clip(jax.random.normal(pieces[3], (SEQ, HEADS, RANK), jnp.float32), -4.0, 4.0)
    iquery = jnp.clip(jax.random.normal(pieces[4], (SEQ, IHEADS, IDIM), jnp.float32), -4.0, 4.0)
    return (latent, ikeys, weights, query, iquery)


def draw_latents(key, part):
    return context_draw(key)[0].astype(jnp.bfloat16)


def draw_index_keys(key, part):
    return context_draw(key)[1].astype(jnp.bfloat16)


def draw_head_weights(key, part):
    return context_draw(key)[2]


def draw_queries(key, part):
    return context_draw(key)[3].astype(jnp.bfloat16)


def draw_index_queries(key, part):
    return context_draw(key)[4].astype(jnp.bfloat16)


def setup_inputs(seed: int = 0) -> dict:
    seeds = jax.random.split(jax.random.key(seed), 7)
    return {
        "queries": draw_queries(jax.random.fold_in(seeds[6], 71), 0),
        "latents": draw_latents(jax.random.fold_in(seeds[6], 71), 0),
        "index_queries": draw_index_queries(jax.random.fold_in(seeds[6], 71), 0),
        "index_keys": draw_index_keys(jax.random.fold_in(seeds[6], 71), 0),
        "head_weights": draw_head_weights(jax.random.fold_in(seeds[6], 71), 0),
        "block_pos": jax.random.permutation(seeds[5], BLOCKS).astype(jnp.int32),
    }


SCALE_ATTN = 192.0 ** -0.5
LOSS_SCALE = 1024.0
NEGATIVE = -1.0e30


def positions(block_pos):
    stored = jnp.arange(SEQ, dtype=jnp.int32)
    return block_pos[stored // TOK_DEV] * TOK_DEV + stored % TOK_DEV


def reference(queries, latents, index_queries, index_keys, head_weights, block_pos):
    place = positions(block_pos)
    visible = place[None, :] <= place[:, None]
    index_scale = IDIM ** -0.5
    latent_wide = latents.astype(jnp.float32)
    keys_wide = index_keys.astype(jnp.float32)

    def attend(summed, query_head):
        scores = SCALE_ATTN * jnp.dot(query_head.astype(jnp.float32), latent_wide.T, precision=lax.Precision.HIGHEST)
        scores = jnp.where(visible, scores, NEGATIVE)
        row_top = jnp.max(scores, axis=1, keepdims=True)
        weights = jnp.where(visible, jnp.exp(scores - row_top), 0.0)
        return summed + weights / jnp.sum(weights, axis=1, keepdims=True), None

    target, _ = lax.scan(attend, jnp.zeros((SEQ, SEQ), jnp.float32), jnp.swapaxes(queries, 0, 1))
    target = target / HEADS

    def index_head(summed, inputs):
        query_head, weight = inputs
        dots = jnp.dot(query_head.astype(jnp.float32), keys_wide.T, precision=lax.Precision.HIGHEST)
        return summed + weight[:, None] * jnp.maximum(dots, 0.0) * index_scale, None

    stacked = (jnp.swapaxes(index_queries, 0, 1), head_weights.T)
    index, _ = lax.scan(index_head, jnp.zeros((SEQ, SEQ), jnp.float32), stacked)
    masked = jnp.where(visible, index, NEGATIVE)
    row_top = jnp.max(masked, axis=1, keepdims=True)
    weights = jnp.where(visible, jnp.exp(masked - row_top), 0.0)
    prob = weights / jnp.sum(weights, axis=1, keepdims=True)
    delta = jnp.where(visible, LOSS_SCALE * (prob - target), 0.0).astype(jnp.bfloat16)
    delta_wide = lax.optimization_barrier(delta).astype(jnp.float32)

    def backward(summed, inputs):
        query_head, weight = inputs
        query_wide = query_head.astype(jnp.float32)
        dots = jnp.dot(query_wide, keys_wide.T, precision=lax.Precision.HIGHEST)
        coef = jnp.where(dots > 0.0, delta_wide * weight[:, None] * index_scale, 0.0).astype(jnp.bfloat16)
        coef = lax.optimization_barrier(coef).astype(jnp.float32)
        grad_query = jnp.dot(coef, keys_wide, precision=lax.Precision.HIGHEST)
        return summed + jnp.dot(coef.T, query_wide, precision=lax.Precision.HIGHEST), grad_query

    grad_keys, grad_queries = lax.scan(backward, jnp.zeros((SEQ, IDIM), jnp.float32), stacked)
    return jnp.swapaxes(grad_queries, 0, 1), grad_keys
```

```python
import math

import jax
import jax.numpy as jnp
from jax import lax
from jax.experimental import pallas as pl
from jax.experimental.pallas import tpu as pltpu
from jax.sharding import PartitionSpec as P

SCALE_ATTN = 192.0 ** (-0.5)
LOG2E = math.log2(math.e)
LOSS_SCALE = 1024.0
NEGATIVE = -1e30
KEYS_STEP = 256
F32 = jnp.float32
BF16 = jnp.bfloat16


def positions(block_pos, first, count, rows):
    stored = first + jnp.arange(count, dtype=jnp.int32)
    owner = stored // rows
    blocks = jnp.arange(block_pos.shape[0], dtype=jnp.int32)
    placed = jnp.sum(jnp.where(owner[:, None] == blocks[None, :], block_pos[None, :], 0), axis=1)
    return placed * rows + stored % rows


def nt(a, b):
    return lax.dot_general(a, b, (((1,), (1,)), ((), ())), preferred_element_type=F32)


def nn(a, b):
    return lax.dot_general(a, b, (((1,), (0,)), ((), ())), preferred_element_type=F32)


def kernel(q_ref, iq_ref, iqt_ref, hw_ref, bias_ref, kv_ref, gq_ref, gk_ref, s_ref, m_ref, x_ref, t_ref):
    M = q_ref.shape[0]
    R, S = bias_ref.shape
    W = iq_ref.shape[1]
    heads = M // R
    step = KEYS_STEP
    lanes = step // 128
    tile = 16 * R
    qs = SCALE_ATTN * LOG2E

    def fold(c, _):
        base = pl.multiple_of(c * step, step)
        k = kv_ref[pl.ds(base, step), :W]
        bias = bias_ref[:, pl.ds(base, step)]
        total = jnp.zeros((R, step), F32)
        for g in range(0, M, tile):
            d = nt(iq_ref[g : g + tile, :], k)
            for h in range(tile // R):
                w = hw_ref[g + h * R : g + (h + 1) * R, :]
                total = total + jnp.maximum(d[h * R : (h + 1) * R], 0.0) * jnp.concatenate([w] * lanes, 1)
        x_ref[:, pl.ds(base, step)] = total + bias
        lat = kv_ref[pl.ds(base, step), W:]
        for g in range(0, M, tile):
            d = nt(q_ref[g : g + tile, :], lat)
            for h in range(tile // R):
                rows = slice(g + h * R, g + (h + 1) * R)
                s = d[h * R : (h + 1) * R] * qs + bias
                s_ref[rows, pl.ds(base, step)] = s
                top = m_ref[rows, :]
                for l in range(lanes):
                    top = jnp.maximum(top, s[:, l * 128 : (l + 1) * 128])
                m_ref[rows, :] = top
        return 0

    m_ref[...] = jnp.full(m_ref.shape, NEGATIVE, F32)
    lax.fori_loop(0, S // step, fold, 0)

    def totals(g, _):
        rows = pl.ds(pl.multiple_of(g * 4 * R, 4 * R), 4 * R)
        top = jnp.max(m_ref[rows, :], axis=1, keepdims=True)
        topb = jnp.broadcast_to(top, (4 * R, 128))

        def inner(c, acc):
            base = pl.multiple_of(c * 512, 512)
            for l in range(4):
                acc = acc + jnp.exp2(s_ref[rows, pl.ds(base + l * 128, 128)] - topb)
            return acc

        acc = lax.fori_loop(0, S // 512, inner, jnp.zeros((4 * R, 128), F32))
        total = jnp.sum(acc, axis=1, keepdims=True)
        m_ref[rows, :] = topb + jnp.broadcast_to(jnp.log2(total), (4 * R, 128))
        return 0

    lax.fori_loop(0, heads // 4, totals, 0)

    def targets(c, _):
        base = pl.multiple_of(c * step, step)
        acc = [jnp.zeros((R, 128), F32) for _ in range(lanes)]
        for h in range(heads):
            rows = slice(h * R, (h + 1) * R)
            m = m_ref[rows, :]
            for l in range(lanes):
                acc[l] = acc[l] + jnp.exp2(s_ref[rows, pl.ds(base + l * 128, 128)] - m)
        for l in range(lanes):
            t_ref[:, pl.ds(base + l * 128, 128)] = acc[l]
        return 0

    lax.fori_loop(0, S // step, targets, 0)

    x = x_ref[...]
    e = jnp.exp(x - jnp.max(x, axis=1, keepdims=True))
    prob = e * (1.0 / jnp.sum(e, axis=1, keepdims=True))
    delta = jnp.where(bias_ref[...] == 0.0, LOSS_SCALE * (prob - t_ref[...] * (1.0 / heads)), 0.0)
    t_ref[...] = delta.astype(BF16).astype(F32)
    s_ref[:, :W] = jnp.zeros((M, W), F32)

    def back(c, _):
        base = pl.multiple_of(c * step, step)
        k = kv_ref[pl.ds(base, step), :W]
        delta = t_ref[:, pl.ds(base, step)]
        gk = jnp.zeros((W, step), F32)
        for g in range(0, M, tile):
            d = nt(iq_ref[g : g + tile, :], k)
            parts = []
            for h in range(tile // R):
                w = hw_ref[g + h * R : g + (h + 1) * R, :]
                parts.append(
                    jnp.where(d[h * R : (h + 1) * R] > 0.0, delta * jnp.concatenate([w] * lanes, 1), 0.0).astype(BF16)
                )
            coef = jnp.concatenate(parts, 0)
            gk = gk + nn(iqt_ref[:, g : g + tile], coef)
            s_ref[g : g + tile, :W] += nn(coef, k)
        gk_ref[pl.ds(base, step), :] = jnp.transpose(gk).astype(BF16)
        return 0

    lax.fori_loop(0, S // step, back, 0)
    gq_ref[...] = s_ref[:, :W].astype(BF16)


def body(queries, latents, index_queries, index_keys, head_weights, block_pos):
    rows = queries.shape[0]
    peers = lax.axis_size("head")
    ctx = lax.axis_size("ctx")
    held = queries.shape[1]
    R = rows // peers
    M = R * held * peers
    W = index_queries.shape[2]
    S = rows * ctx

    kv = lax.all_gather(jnp.concatenate([index_keys, latents], 1), "ctx", axis=0, tiled=True)

    def to_rows(a):
        a = jnp.transpose(a.reshape(peers, R, held, -1), (0, 2, 1, 3))
        a = lax.all_to_all(a, "head", split_axis=0, concat_axis=0, tiled=True)
        return a.reshape(M, -1)

    iq = to_rows(index_queries)
    q = to_rows(queries)
    hw = to_rows(head_weights[:, :, None]) * (W ** (-0.5))
    hw = jnp.broadcast_to(hw, (M, 128))

    first = lax.axis_index("ctx") * rows + lax.axis_index("head") * R
    query_pos = positions(block_pos, first, R, rows)
    key_pos = positions(block_pos, jnp.int32(0), S, rows)
    bias = jnp.where(key_pos[None, :] <= query_pos[:, None], 0.0, NEGATIVE).astype(F32)

    gq, gk = pl.pallas_call(
        kernel,
        out_shape=(jax.ShapeDtypeStruct((M, W), BF16), jax.ShapeDtypeStruct((S, W), BF16)),
        scratch_shapes=[
            pltpu.VMEM((M, S), F32),
            pltpu.VMEM((M, 128), F32),
            pltpu.VMEM((R, S), F32),
            pltpu.VMEM((R, S), F32),
        ],
        compiler_params=pltpu.CompilerParams(vmem_limit_bytes=60 << 20),
        name="indexer",
    )(q, iq, jnp.transpose(iq), hw, bias, kv)

    gk = lax.all_to_all(gk.reshape(ctx, rows, W), "ctx", split_axis=0, concat_axis=0, tiled=True)
    gk = jnp.sum(gk.astype(F32), axis=0).astype(BF16)
    last = jnp.concatenate(
        [gq.reshape(peers, M // peers, W), jnp.broadcast_to(gk[None], (peers, rows, W))], 1
    )
    last = lax.all_to_all(last, "head", split_axis=0, concat_axis=0, tiled=True)
    gq = last[:, : M // peers].reshape(peers, held, R, W)
    gq = jnp.transpose(gq, (0, 2, 1, 3)).reshape(rows, held, W).astype(F32)
    gk = jnp.sum(last[:, M // peers :].astype(F32), axis=0)
    return gq, gk


def solution(mesh):
    return jax.shard_map(
        body,
        mesh=mesh,
        in_specs=(
            P("ctx", "head", None),
            P("ctx", None),
            P("ctx", "head", None),
            P("ctx", None),
            P("ctx", "head"),
            P(),
        ),
        out_specs=(P("ctx", "head", None), P("ctx", None)),
        check_vma=False,
    )
```

```python
import math

import jax
import jax.numpy as jnp
from jax import lax
from jax.experimental import pallas as pl
from jax.experimental.pallas import tpu as pltpu
from jax.sharding import Mesh
from jax.sharding import PartitionSpec as P

SCALE_ATTN = 192.0 ** (-0.5)
LOG2E = math.log2(math.e)
LOSS_SCALE = 1024.0
NEGATIVE = -1e30
KEYS_STEP = 256
F32 = jnp.float32
BF16 = jnp.bfloat16


def nt(a, b):
    return lax.dot_general(a, b, (((1,), (1,)), ((), ())), preferred_element_type=F32)


def nn(a, b):
    return lax.dot_general(a, b, (((1,), (0,)), ((), ())), preferred_element_type=F32)


def kernel(offs_ref, p_ref, iqt_ref, hw_ref, bias_ref, kva_ref, kvb_ref, gq_ref, gka_ref, gkb_ref, s_ref, m_ref, x_ref, t_ref):
    M = p_ref.shape[0]
    R, S = bias_ref.shape
    W = iqt_ref.shape[0]
    heads = M // R
    step = KEYS_STEP
    lanes = step // 128
    tile = 16 * R
    half = kva_ref.shape[0]
    wide = kva_ref.shape[1]
    chunk = half // offs_ref.shape[0]
    qs = SCALE_ATTN * LOG2E

    m_ref[...] = jnp.full(m_ref.shape, NEGATIVE, F32)
    for part, kv_ref in enumerate((kva_ref, kvb_ref)):

        def fold(c, _):
            here = pl.multiple_of(c * step, step)
            base = pl.multiple_of(part * half + c * step, step)
            k = kv_ref[pl.ds(here, step), :W]
            bias = bias_ref[:, pl.ds(base, step)]
            total = jnp.zeros((R, step), F32)
            for g in range(0, M, tile):
                d = nt(p_ref[g : g + tile, :W], k)
                for h in range(tile // R):
                    w = hw_ref[g + h * R : g + (h + 1) * R, :]
                    total = total + jnp.maximum(d[h * R : (h + 1) * R], 0.0) * jnp.concatenate([w] * lanes, 1)
            x_ref[:, pl.ds(base, step)] = total + bias
            lat = kv_ref[pl.ds(here, step), W:]
            for g in range(0, M, tile):
                d = nt(p_ref[g : g + tile, W:wide], lat)
                for h in range(tile // R):
                    rows = slice(g + h * R, g + (h + 1) * R)
                    s = d[h * R : (h + 1) * R] * qs + bias
                    s_ref[rows, pl.ds(base, step)] = s
                    top = m_ref[rows, :]
                    for l in range(lanes):
                        top = jnp.maximum(top, s[:, l * 128 : (l + 1) * 128])
                    m_ref[rows, :] = top
            return 0

        lax.fori_loop(0, half // step, fold, 0)

    def totals(g, _):
        rows = pl.ds(pl.multiple_of(g * 4 * R, 4 * R), 4 * R)
        top = jnp.max(m_ref[rows, :], axis=1, keepdims=True)
        topb = jnp.broadcast_to(top, (4 * R, 128))

        def inner(c, acc):
            base = pl.multiple_of(c * 512, 512)
            for l in range(4):
                acc = acc + jnp.exp2(s_ref[rows, pl.ds(base + l * 128, 128)] - topb)
            return acc

        acc = lax.fori_loop(0, S // 512, inner, jnp.zeros((4 * R, 128), F32))
        total = jnp.sum(acc, axis=1, keepdims=True)
        m_ref[rows, :] = topb + jnp.broadcast_to(jnp.log2(total), (4 * R, 128))
        return 0

    lax.fori_loop(0, heads // 4, totals, 0)

    def targets(c, _):
        base = pl.multiple_of(c * step, step)
        acc = [jnp.zeros((R, 128), F32) for _ in range(lanes)]
        for h in range(heads):
            rows = slice(h * R, (h + 1) * R)
            m = m_ref[rows, :]
            for l in range(lanes):
                acc[l] = acc[l] + jnp.exp2(s_ref[rows, pl.ds(base + l * 128, 128)] - m)
        for l in range(lanes):
            t_ref[:, pl.ds(base + l * 128, 128)] = acc[l]
        return 0

    lax.fori_loop(0, S // step, targets, 0)

    x = x_ref[...]
    e = jnp.exp(x - jnp.max(x, axis=1, keepdims=True))
    prob = e * (1.0 / jnp.sum(e, axis=1, keepdims=True))
    delta = jnp.where(bias_ref[...] == 0.0, LOSS_SCALE * (prob - t_ref[...] * (1.0 / heads)), 0.0)
    t_ref[...] = delta.astype(BF16).astype(F32)
    s_ref[:, :W] = jnp.zeros((M, W), F32)

    for part, (kv_ref, gk_ref) in enumerate(((kva_ref, gka_ref), (kvb_ref, gkb_ref))):

        def back(c, _):
            here = pl.multiple_of(c * step, step)
            base = pl.multiple_of(part * half + c * step, step)
            k = kv_ref[pl.ds(here, step), :W]
            delta = t_ref[:, pl.ds(base, step)]
            gk = jnp.zeros((W, step), F32)
            for g in range(0, M, tile):
                d = nt(p_ref[g : g + tile, :W], k)
                parts = []
                for h in range(tile // R):
                    w = hw_ref[g + h * R : g + (h + 1) * R, :]
                    parts.append(
                        jnp.where(d[h * R : (h + 1) * R] > 0.0, delta * jnp.concatenate([w] * lanes, 1), 0.0).astype(BF16)
                    )
                coef = jnp.concatenate(parts, 0)
                gk = gk + nn(iqt_ref[:, g : g + tile], coef)
                s_ref[g : g + tile, :W] += nn(coef, k)
            gk = jnp.transpose(gk).astype(BF16)
            for e in range(step // chunk):
                off = pl.multiple_of(offs_ref[c * (step // chunk) + e], chunk)
                gk_ref[pl.ds(off, chunk), :] = gk[e * chunk : (e + 1) * chunk]
            return 0

        lax.fori_loop(0, half // step, back, 0)
    gq_ref[...] = s_ref[:, :W].astype(BF16)


def shifted(sizes, axis, by):
    total = sizes[0] * sizes[1]
    pairs = []
    for i in range(total):
        a, b = divmod(i, sizes[1])
        a, b = ((a + by) % sizes[0], b) if axis == 0 else (a, (b + by) % sizes[1])
        pairs.append((i, a * sizes[1] + b))
    return pairs


def make_body(xs, zs, ys, zls):
    def body(queries, latents, index_queries, index_keys, head_weights, block_pos):
        rows = queries.shape[0]
        peers = lax.axis_size("head")
        held = queries.shape[1]
        R = rows // peers
        M = R * held * peers
        W = index_queries.shape[2]
        quarter = rows // ys
        xz = lax.axis_index("xz")
        core = lax.axis_index("core")
        head = lax.axis_index("head")
        x, z, y = xz // zs, xz % zs, head % ys

        def along_x(a, by):
            return lax.ppermute(a, "xz", shifted((xs, zs), 0, by)) if by else a

        def along_z(a, by):
            return lax.ppermute(a, "xz", shifted((xs, zs), 1, by)) if by else a

        def along_y(a, by):
            return lax.ppermute(a, "head", shifted((zls, ys), 1, by)) if by else a

        own = jnp.concatenate([index_keys, latents], 1)
        piece = lax.dynamic_slice_in_dim(own, y * quarter, quarter, 0)
        from_z = jnp.concatenate([along_z(piece, d) for d in range(1, zs)], 0)
        col = jnp.concatenate([along_x(piece, d) for d in range(xs)], 0)
        row = jnp.concatenate([along_y(from_z, d) for d in range(ys)], 0)
        kva = jnp.concatenate([along_y(col, d) for d in range(ys)] + [along_x(row, d) for d in range(xs)], 0)
        kvb = lax.ppermute(kva, "core", [(0, 1), (1, 0)])

        order = [(dx, 0, dy) for dy in range(ys) for dx in range(xs)]
        order += [(dx, dz, dy) for dx in range(xs) for dy in range(ys) for dz in range(1, zs)]
        order = jnp.array(order, jnp.int32)
        ox = (x - order[:, 0]) % xs
        oz = (z - order[:, 1]) % zs
        oy = (y - order[:, 2]) % ys
        offs = (ox * zs + oz) * rows + oy * quarter
        blocks = jnp.concatenate([(ox * zs + oz) * 2 + core, (ox * zs + oz) * 2 + 1 - core])
        ids = jnp.arange(block_pos.shape[0], dtype=jnp.int32)

        def place(block):
            return jnp.sum(jnp.where(block[:, None] == ids[None, :], block_pos[None, :], 0), axis=1) * rows

        key_pos = place(blocks) + jnp.concatenate([oy, oy]) * quarter
        key_pos = (key_pos[:, None] + jnp.arange(quarter, dtype=jnp.int32)[None, :]).reshape(-1)
        query_pos = place((xz * 2 + core)[None]) + head * R + jnp.arange(R, dtype=jnp.int32)
        bias = jnp.where(key_pos[None, :] <= query_pos[:, None], 0.0, NEGATIVE).astype(F32)
        S = key_pos.shape[0]

        hi = lax.reduce_precision(head_weights, 8, 7)
        rest = head_weights - hi
        mid = lax.reduce_precision(rest, 8, 7)
        pieces = jnp.stack([hi, mid, rest - mid], 2).astype(BF16)
        packed = jnp.concatenate([index_queries, queries, pieces], 2)
        packed = jnp.transpose(packed.reshape(peers, R, held, -1), (0, 2, 1, 3))
        packed = lax.all_to_all(packed, "head", split_axis=0, concat_axis=0, tiled=True).reshape(M, -1)
        hw = jnp.sum(packed[:, -3:].astype(F32), axis=1, keepdims=True) * (W ** (-0.5))
        hw = jnp.broadcast_to(hw, (M, 128))

        vmem = pl.BlockSpec(memory_space=pltpu.VMEM)
        gq, gka, gkb = pl.pallas_call(
            kernel,
            in_specs=[pl.BlockSpec(memory_space=pltpu.SMEM)] + [vmem] * 6,
            out_specs=(vmem, vmem, vmem),
            out_shape=(
                jax.ShapeDtypeStruct((M, W), BF16),
                jax.ShapeDtypeStruct((S // 2, W), BF16),
                jax.ShapeDtypeStruct((S // 2, W), BF16),
            ),
            scratch_shapes=[
                pltpu.VMEM((M, S), F32),
                pltpu.VMEM((M, 128), F32),
                pltpu.VMEM((R, S), F32),
                pltpu.VMEM((R, S), F32),
            ],
            compiler_params=pltpu.CompilerParams(vmem_limit_bytes=60 << 20),
            name="indexer",
        )(offs, packed, jnp.transpose(packed[:, :W]), hw, bias, kva, kvb)

        gkb = lax.ppermute(gkb, "core", [(0, 1), (1, 0)])
        gk = (gka.astype(F32) + gkb.astype(F32)).astype(BF16).reshape(xs * zs, rows, W)
        gk = lax.all_to_all(gk, "xz", split_axis=0, concat_axis=0, tiled=True)
        gk = jnp.sum(gk.astype(F32), axis=0).astype(BF16)
        last = jnp.concatenate(
            [gq.reshape(peers, M // peers, W), jnp.broadcast_to(gk[None], (peers, rows, W))], 1
        )
        last = lax.all_to_all(last, "head", split_axis=0, concat_axis=0, tiled=True)
        gq = last[:, : M // peers].reshape(peers, held, R, W)
        gq = jnp.transpose(gq, (0, 2, 1, 3)).reshape(rows, held, W).astype(F32)
        gk = jnp.sum(last[:, M // peers :].astype(F32), axis=0)
        return gq, gk

    return body


def solution(mesh):
    xs, zs, cores, zls, ys = 4, 4, 2, 2, 4
    grid = Mesh(mesh.devices.reshape(xs * zs, cores, zls * ys), ("xz", "core", "head"))
    ctx = ("xz", "core")
    return jax.shard_map(
        make_body(xs, zs, ys, zls),
        mesh=grid,
        in_specs=(
            P(ctx, "head", None),
            P(ctx, None),
            P(ctx, "head", None),
            P(ctx, None),
            P(ctx, "head"),
            P(),
        ),
        out_specs=(P(ctx, "head", None), P(ctx, None)),
        check_vma=False,
    )
```

```python
import math

import jax
import jax.numpy as jnp
from jax import lax
from jax.experimental import pallas as pl
from jax.experimental.pallas import tpu as pltpu
from jax.sharding import Mesh
from jax.sharding import PartitionSpec as P

SCALE_ATTN = 192.0 ** (-0.5)
LOG2E = math.log2(math.e)
LOSS_SCALE = 1024.0
NEGATIVE = -1e30
KEYS_STEP = 256
F32 = jnp.float32
BF16 = jnp.bfloat16


def nt(a, b):
    return lax.dot_general(a, b, (((1,), (1,)), ((), ())), preferred_element_type=F32)


def nn(a, b):
    return lax.dot_general(a, b, (((1,), (0,)), ((), ())), preferred_element_type=F32)


def kernel(offs_ref, p_ref, iqt_ref, hw_ref, bias_ref, kva_ref, kvb_ref, gq_ref, gka_ref, gkb_ref, s_ref, m_ref, x_ref, t_ref):
    M = p_ref.shape[0]
    R, S = bias_ref.shape
    W = iqt_ref.shape[0]
    heads = M // R
    step = KEYS_STEP
    lanes = step // 128
    tile = 16 * R
    half = kva_ref.shape[0]
    wide = kva_ref.shape[1]
    chunk = half // offs_ref.shape[0]
    qs = SCALE_ATTN * LOG2E

    m_ref[...] = jnp.full(m_ref.shape, NEGATIVE, F32)
    for part, kv_ref in enumerate((kva_ref, kvb_ref)):

        def fold(c, _):
            here = pl.multiple_of(c * step, step)
            base = pl.multiple_of(part * half + c * step, step)
            k = kv_ref[pl.ds(here, step), :W]
            bias = bias_ref[:, pl.ds(base, step)]
            total = jnp.zeros((R, step), F32)
            for g in range(0, M, tile):
                d = nt(p_ref[g : g + tile, :W], k)
                for h in range(tile // R):
                    w = hw_ref[g + h * R : g + (h + 1) * R, :]
                    total = total + jnp.maximum(d[h * R : (h + 1) * R], 0.0) * jnp.concatenate([w] * lanes, 1)
            x_ref[:, pl.ds(base, step)] = total + bias
            lat = kv_ref[pl.ds(here, step), W:]
            for g in range(0, M, tile):
                d = nt(p_ref[g : g + tile, W:wide], lat)
                for h in range(tile // R):
                    rows = slice(g + h * R, g + (h + 1) * R)
                    s = d[h * R : (h + 1) * R] * qs + bias
                    s_ref[rows, pl.ds(base, step)] = s
                    top = m_ref[rows, :]
                    for l in range(lanes):
                        top = jnp.maximum(top, s[:, l * 128 : (l + 1) * 128])
                    m_ref[rows, :] = top
            return 0

        lax.fori_loop(0, half // step, fold, 0)

    def totals(g, _):
        rows = pl.ds(pl.multiple_of(g * 4 * R, 4 * R), 4 * R)
        top = jnp.max(m_ref[rows, :], axis=1, keepdims=True)
        topb = jnp.broadcast_to(top, (4 * R, 128))

        def inner(c, acc):
            base = pl.multiple_of(c * 512, 512)
            for l in range(4):
                acc = acc + jnp.exp2(s_ref[rows, pl.ds(base + l * 128, 128)] - topb)
            return acc

        acc = lax.fori_loop(0, S // 512, inner, jnp.zeros((4 * R, 128), F32))
        total = jnp.sum(acc, axis=1, keepdims=True)
        m_ref[rows, :] = topb + jnp.broadcast_to(jnp.log2(total), (4 * R, 128))
        return 0

    lax.fori_loop(0, heads // 4, totals, 0)

    def targets(c, _):
        base = pl.multiple_of(c * step, step)
        acc = [jnp.zeros((R, 128), F32) for _ in range(lanes)]
        for h in range(heads):
            rows = slice(h * R, (h + 1) * R)
            m = m_ref[rows, :]
            for l in range(lanes):
                acc[l] = acc[l] + jnp.exp2(s_ref[rows, pl.ds(base + l * 128, 128)] - m)
        for l in range(lanes):
            t_ref[:, pl.ds(base + l * 128, 128)] = acc[l]
        return 0

    lax.fori_loop(0, S // step, targets, 0)

    x = x_ref[...]
    e = jnp.exp(x - jnp.max(x, axis=1, keepdims=True))
    prob = e * (1.0 / jnp.sum(e, axis=1, keepdims=True))
    delta = jnp.where(bias_ref[...] == 0.0, LOSS_SCALE * (prob - t_ref[...] * (1.0 / heads)), 0.0)
    t_ref[...] = delta.astype(BF16).astype(F32)
    s_ref[:, :W] = jnp.zeros((M, W), F32)

    for part, (kv_ref, gk_ref) in enumerate(((kva_ref, gka_ref), (kvb_ref, gkb_ref))):

        def back(c, _):
            here = pl.multiple_of(c * step, step)
            base = pl.multiple_of(part * half + c * step, step)
            k = kv_ref[pl.ds(here, step), :W]
            delta = t_ref[:, pl.ds(base, step)]
            gk = jnp.zeros((W, step), F32)
            for g in range(0, M, tile):
                d = nt(p_ref[g : g + tile, :W], k)
                parts = []
                for h in range(tile // R):
                    w = hw_ref[g + h * R : g + (h + 1) * R, :]
                    parts.append(
                        jnp.where(d[h * R : (h + 1) * R] > 0.0, delta * jnp.concatenate([w] * lanes, 1), 0.0).astype(BF16)
                    )
                coef = jnp.concatenate(parts, 0)
                gk = gk + nn(iqt_ref[:, g : g + tile], coef)
                s_ref[g : g + tile, :W] += nn(coef, k)
            gk = jnp.transpose(gk).astype(BF16)
            for e in range(step // chunk):
                off = pl.multiple_of(offs_ref[c * (step // chunk) + e], chunk)
                gk_ref[pl.ds(off, chunk), :] = gk[e * chunk : (e + 1) * chunk]
            return 0

        lax.fori_loop(0, half // step, back, 0)
    gq_ref[...] = s_ref[:, :W].astype(BF16)


def shifted(sizes, axis, by):
    total = sizes[0] * sizes[1]
    pairs = []
    for i in range(total):
        a, b = divmod(i, sizes[1])
        a, b = ((a + by) % sizes[0], b) if axis == 0 else (a, (b + by) % sizes[1])
        pairs.append((i, a * sizes[1] + b))
    return pairs


def make_body(xs, zs, ys, zls):
    def body(queries, latents, index_queries, index_keys, head_weights, block_pos):
        rows = queries.shape[0]
        peers = lax.axis_size("head")
        held = queries.shape[1]
        R = rows // peers
        M = R * held * peers
        W = index_queries.shape[2]
        quarter = rows // ys
        xz = lax.axis_index("xz")
        core = lax.axis_index("core")
        head = lax.axis_index("head")
        x, z, y = xz // zs, xz % zs, head % ys

        def along_x(a, by):
            return lax.ppermute(a, "xz", shifted((xs, zs), 0, by)) if by else a

        def along_z(a, by):
            return lax.ppermute(a, "xz", shifted((xs, zs), 1, by)) if by else a

        def along_y(a, by):
            return lax.ppermute(a, "head", shifted((zls, ys), 1, by)) if by else a

        width = W + latents.shape[1]
        spare = -width % 128
        own = jnp.concatenate([index_keys, latents, jnp.zeros((rows, spare), BF16)], 1)
        piece = lax.dynamic_slice_in_dim(own, y * quarter, quarter, 0)
        from_z = jnp.concatenate([along_z(piece, d) for d in range(1, zs)], 0)
        col = jnp.concatenate([along_x(piece, d) for d in range(xs)], 0)
        hi = lax.reduce_precision(head_weights, 8, 7)
        rest = head_weights - hi
        mid = lax.reduce_precision(rest, 8, 7)
        pieces = jnp.stack([hi, mid, rest - mid], 2).astype(BF16)
        unused = jnp.zeros((rows, held, spare - 3), BF16)
        packed = jnp.concatenate([index_queries, queries, pieces, unused], 2)
        packed = jnp.transpose(packed.reshape(peers, R, held, -1), (0, 2, 1, 3))
        from_z, packed = lax.optimization_barrier((from_z, packed))
        packed = lax.all_to_all(packed, "head", split_axis=0, concat_axis=0, tiled=True).reshape(M, -1)
        row = jnp.concatenate([along_y(from_z, d) for d in range(ys)], 0)
        kva = jnp.concatenate([along_y(col, d) for d in range(ys)] + [along_x(row, d) for d in range(xs)], 0)
        kvb = lax.ppermute(kva, "core", [(0, 1), (1, 0)])

        order = [(dx, 0, dy) for dy in range(ys) for dx in range(xs)]
        order += [(dx, dz, dy) for dx in range(xs) for dy in range(ys) for dz in range(1, zs)]
        order = jnp.array(order, jnp.int32)
        ox = (x - order[:, 0]) % xs
        oz = (z - order[:, 1]) % zs
        oy = (y - order[:, 2]) % ys
        offs = (ox * zs + oz) * rows + oy * quarter
        blocks = jnp.concatenate([(ox * zs + oz) * 2 + core, (ox * zs + oz) * 2 + 1 - core])
        ids = jnp.arange(block_pos.shape[0], dtype=jnp.int32)

        def place(block):
            return jnp.sum(jnp.where(block[:, None] == ids[None, :], block_pos[None, :], 0), axis=1) * rows

        key_pos = place(blocks) + jnp.concatenate([oy, oy]) * quarter
        key_pos = (key_pos[:, None] + jnp.arange(quarter, dtype=jnp.int32)[None, :]).reshape(-1)
        query_pos = place((xz * 2 + core)[None]) + head * R + jnp.arange(R, dtype=jnp.int32)
        bias = jnp.where(key_pos[None, :] <= query_pos[:, None], 0.0, NEGATIVE).astype(F32)
        S = key_pos.shape[0]

        hw = jnp.sum(packed[:, width : width + 3].astype(F32), axis=1, keepdims=True) * (W ** (-0.5))
        hw = jnp.broadcast_to(hw, (M, 128))

        vmem = pl.BlockSpec(memory_space=pltpu.VMEM)
        gq, gka, gkb = pl.pallas_call(
            kernel,
            in_specs=[pl.BlockSpec(memory_space=pltpu.SMEM)] + [vmem] * 6,
            out_specs=(vmem, vmem, vmem),
            out_shape=(
                jax.ShapeDtypeStruct((M, W), BF16),
                jax.ShapeDtypeStruct((S // 2, W), BF16),
                jax.ShapeDtypeStruct((S // 2, W), BF16),
            ),
            scratch_shapes=[
                pltpu.VMEM((M, S), F32),
                pltpu.VMEM((M, 128), F32),
                pltpu.VMEM((R, S), F32),
                pltpu.VMEM((R, S), F32),
            ],
            compiler_params=pltpu.CompilerParams(vmem_limit_bytes=60 << 20),
            name="indexer",
        )(offs, packed, jnp.transpose(packed[:, :W]), hw, bias, kva, kvb)

        gkb = lax.ppermute(gkb, "core", [(0, 1), (1, 0)])
        gk = (gka.astype(F32) + gkb.astype(F32)).astype(BF16).reshape(xs * zs, rows, W)
        gk = lax.all_to_all(gk, "xz", split_axis=0, concat_axis=0, tiled=True)
        gk = jnp.sum(gk.astype(F32), axis=0).astype(BF16)
        last = jnp.concatenate(
            [gq.reshape(peers, M // peers, W), jnp.broadcast_to(gk[None], (peers, rows, W))], 1
        )
        last = lax.all_to_all(last, "head", split_axis=0, concat_axis=0, tiled=True)
        gq = last[:, : M // peers].reshape(peers, held, R, W)
        gq = jnp.transpose(gq, (0, 2, 1, 3)).reshape(rows, held, W).astype(F32)
        gk = jnp.sum(last[:, M // peers :].astype(F32), axis=0)
        return gq, gk

    return body


def solution(mesh):
    xs, zs, cores, zls, ys = 4, 4, 2, 2, 4
    grid = Mesh(mesh.devices.reshape(xs * zs, cores, zls * ys), ("xz", "core", "head"))
    ctx = ("xz", "core")
    return jax.shard_map(
        make_body(xs, zs, ys, zls),
        mesh=grid,
        in_specs=(
            P(ctx, "head", None),
            P(ctx, None),
            P(ctx, "head", None),
            P(ctx, None),
            P(ctx, "head"),
            P(),
        ),
        out_specs=(P(ctx, "head", None), P(ctx, None)),
        check_vma=False,
    )
```

```python
import math

import jax
import jax.numpy as jnp
from jax import lax
from jax.experimental import pallas as pl
from jax.experimental.pallas import tpu as pltpu
from jax.sharding import Mesh
from jax.sharding import PartitionSpec as P

SCALE_ATTN = 192.0 ** (-0.5)
LOG2E = math.log2(math.e)
LOSS_SCALE = 1024.0
NEGATIVE = -1e30
KEYS_STEP = 256
F32 = jnp.float32
BF16 = jnp.bfloat16


def nt(a, b):
    return lax.dot_general(a, b, (((1,), (1,)), ((), ())), preferred_element_type=F32)


def nn(a, b):
    return lax.dot_general(a, b, (((1,), (0,)), ((), ())), preferred_element_type=F32)


def kernel(offs_ref, p_ref, iqt_ref, hw_ref, bias_ref, kva_ref, kvb_ref, gq_ref, gka_ref, gkb_ref, s_ref, m_ref, x_ref, t_ref, c_ref):
    M = p_ref.shape[0]
    R, S = bias_ref.shape
    W = iqt_ref.shape[0]
    heads = M // R
    step = KEYS_STEP
    lanes = step // 128
    tile = 16 * R
    half = kva_ref.shape[0]
    wide = kva_ref.shape[1]
    chunk = half // offs_ref.shape[0]
    qs = SCALE_ATTN * LOG2E

    m_ref[...] = jnp.full(m_ref.shape, NEGATIVE, F32)
    for part, kv_ref in enumerate((kva_ref, kvb_ref)):

        def fold(c, _):
            here = pl.multiple_of(c * step, step)
            base = pl.multiple_of(part * half + c * step, step)
            k = kv_ref[pl.ds(here, step), :W]
            bias = bias_ref[:, pl.ds(base, step)]
            total = jnp.zeros((R, step), F32)
            for g in range(0, M, tile):
                d = nt(p_ref[g : g + tile, :W], k)
                c_ref[g : g + tile, pl.ds(base, step)] = d.astype(BF16)
                for h in range(tile // R):
                    w = hw_ref[g + h * R : g + (h + 1) * R, :]
                    total = total + jnp.maximum(d[h * R : (h + 1) * R], 0.0) * jnp.concatenate([w] * lanes, 1)
            x_ref[:, pl.ds(base, step)] = total + bias
            lat = kv_ref[pl.ds(here, step), W:]
            for g in range(0, M, tile):
                d = nt(p_ref[g : g + tile, W:wide], lat)
                for h in range(tile // R):
                    rows = slice(g + h * R, g + (h + 1) * R)
                    s = d[h * R : (h + 1) * R] * qs + bias
                    s_ref[rows, pl.ds(base, step)] = s
                    top = m_ref[rows, :]
                    for l in range(lanes):
                        top = jnp.maximum(top, s[:, l * 128 : (l + 1) * 128])
                    m_ref[rows, :] = top
            return 0

        lax.fori_loop(0, half // step, fold, 0)

    def totals(g, _):
        rows = pl.ds(pl.multiple_of(g * 4 * R, 4 * R), 4 * R)
        top = jnp.max(m_ref[rows, :], axis=1, keepdims=True)
        topb = jnp.broadcast_to(top, (4 * R, 128))

        def inner(c, acc):
            base = pl.multiple_of(c * 2048, 2048)
            for l in range(16):
                acc = acc + jnp.exp2(s_ref[rows, pl.ds(base + l * 128, 128)] - topb)
            return acc

        acc = lax.fori_loop(0, S // 2048, inner, jnp.zeros((4 * R, 128), F32))
        total = jnp.sum(acc, axis=1, keepdims=True)
        m_ref[rows, :] = topb + jnp.broadcast_to(jnp.log2(total), (4 * R, 128))
        return 0

    lax.fori_loop(0, heads // 4, totals, 0)

    def targets(c, _):
        base = pl.multiple_of(c * step, step)
        acc = [jnp.zeros((R, 128), F32) for _ in range(lanes)]
        for h in range(heads):
            rows = slice(h * R, (h + 1) * R)
            m = m_ref[rows, :]
            for l in range(lanes):
                acc[l] = acc[l] + jnp.exp2(s_ref[rows, pl.ds(base + l * 128, 128)] - m)
        for l in range(lanes):
            t_ref[:, pl.ds(base + l * 128, 128)] = acc[l]
        return 0

    lax.fori_loop(0, S // step, targets, 0)

    x = x_ref[...]
    e = jnp.exp(x - jnp.max(x, axis=1, keepdims=True))
    prob = e * (1.0 / jnp.sum(e, axis=1, keepdims=True))
    delta = jnp.where(bias_ref[...] == 0.0, LOSS_SCALE * (prob - t_ref[...] * (1.0 / heads)), 0.0)
    t_ref[...] = delta.astype(BF16).astype(F32)

    def coefs(c, _):
        base = pl.multiple_of(c * step, step)
        delta = t_ref[:, pl.ds(base, step)]
        for h in range(heads):
            rows = slice(h * R, (h + 1) * R)
            w = hw_ref[rows, :]
            d = c_ref[rows, pl.ds(base, step)]
            value = (delta * jnp.concatenate([w] * lanes, 1)).astype(BF16)
            c_ref[rows, pl.ds(base, step)] = jnp.where(d > 0, value, jnp.zeros_like(value))
        return 0

    lax.fori_loop(0, S // step, coefs, 0)

    wide_step = 4 * step
    for part, gk_ref in enumerate((gka_ref, gkb_ref)):

        def keys(c, _):
            base = pl.multiple_of(part * half + c * wide_step, wide_step)
            gk = nn(iqt_ref[...], c_ref[:, pl.ds(base, wide_step)])
            gk = jnp.transpose(gk).astype(BF16)
            for e in range(wide_step // chunk):
                off = pl.multiple_of(offs_ref[c * (wide_step // chunk) + e], chunk)
                gk_ref[pl.ds(off, chunk), :] = gk[e * chunk : (e + 1) * chunk]
            return 0

        lax.fori_loop(0, half // wide_step, keys, 0)

    def index_queries(g, _):
        rows = pl.ds(pl.multiple_of(g * tile, tile), tile)
        gq = nn(c_ref[rows, :half], kva_ref[:, :W]) + nn(c_ref[rows, half:], kvb_ref[:, :W])
        gq_ref[rows, :] = gq.astype(BF16)
        return 0

    lax.fori_loop(0, M // tile, index_queries, 0)


def shifted(sizes, axis, by):
    total = sizes[0] * sizes[1]
    pairs = []
    for i in range(total):
        a, b = divmod(i, sizes[1])
        a, b = ((a + by) % sizes[0], b) if axis == 0 else (a, (b + by) % sizes[1])
        pairs.append((i, a * sizes[1] + b))
    return pairs


def make_body(xs, zs, ys, zls):
    def body(queries, latents, index_queries, index_keys, head_weights, block_pos):
        rows = queries.shape[0]
        peers = lax.axis_size("head")
        held = queries.shape[1]
        R = rows // peers
        M = R * held * peers
        W = index_queries.shape[2]
        quarter = rows // ys
        xz = lax.axis_index("xz")
        core = lax.axis_index("core")
        head = lax.axis_index("head")
        x, z, y = xz // zs, xz % zs, head % ys

        def along_x(a, by):
            return lax.ppermute(a, "xz", shifted((xs, zs), 0, by)) if by else a

        def along_z(a, by):
            return lax.ppermute(a, "xz", shifted((xs, zs), 1, by)) if by else a

        def along_y(a, by):
            return lax.ppermute(a, "head", shifted((zls, ys), 1, by)) if by else a

        width = W + latents.shape[1]
        spare = -width % 128
        own = jnp.concatenate([index_keys, latents, jnp.zeros((rows, spare), BF16)], 1)
        piece = lax.dynamic_slice_in_dim(own, y * quarter, quarter, 0)
        from_z = jnp.concatenate([along_z(piece, d) for d in range(1, zs)], 0)
        col = jnp.concatenate([along_x(piece, d) for d in range(xs)], 0)
        hi = lax.reduce_precision(head_weights, 8, 7)
        rest = head_weights - hi
        mid = lax.reduce_precision(rest, 8, 7)
        pieces = jnp.stack([hi, mid, rest - mid], 2).astype(BF16)
        unused = jnp.zeros((rows, held, spare - 3), BF16)
        packed = jnp.concatenate([index_queries, queries, pieces, unused], 2)
        packed = jnp.transpose(packed.reshape(peers, R, held, -1), (0, 2, 1, 3))
        from_z, packed = lax.optimization_barrier((from_z, packed))
        packed = lax.all_to_all(packed, "head", split_axis=0, concat_axis=0, tiled=True).reshape(M, -1)
        row = jnp.concatenate([along_y(from_z, d) for d in range(ys)], 0)
        kva = [along_y(col, d) for d in range(ys)]
        for d in range(xs):
            kva.append(along_x(row, d))
        kva = jnp.concatenate(kva, 0)
        kvb = lax.ppermute(kva, "core", [(0, 1), (1, 0)])

        order = [(dx, 0, dy) for dy in range(ys) for dx in range(xs)]
        order += [(dx, dz, dy) for dx in range(xs) for dy in range(ys) for dz in range(1, zs)]
        order = jnp.array(order, jnp.int32)
        ox = (x - order[:, 0]) % xs
        oz = (z - order[:, 1]) % zs
        oy = (y - order[:, 2]) % ys
        offs = (ox * zs + oz) * rows + oy * quarter
        blocks = jnp.concatenate([(ox * zs + oz) * 2 + core, (ox * zs + oz) * 2 + 1 - core])
        ids = jnp.arange(block_pos.shape[0], dtype=jnp.int32)

        def place(block):
            return jnp.sum(jnp.where(block[:, None] == ids[None, :], block_pos[None, :], 0), axis=1) * rows

        key_pos = place(blocks) + jnp.concatenate([oy, oy]) * quarter
        key_pos = (key_pos[:, None] + jnp.arange(quarter, dtype=jnp.int32)[None, :]).reshape(-1)
        query_pos = place((xz * 2 + core)[None]) + head * R + jnp.arange(R, dtype=jnp.int32)
        bias = jnp.where(key_pos[None, :] <= query_pos[:, None], 0.0, NEGATIVE).astype(F32)
        S = key_pos.shape[0]

        hw = jnp.sum(packed[:, width : width + 3].astype(F32), axis=1, keepdims=True) * (W ** (-0.5))
        hw = jnp.broadcast_to(hw, (M, 128))

        vmem = pl.BlockSpec(memory_space=pltpu.VMEM)
        gq, gka, gkb = pl.pallas_call(
            kernel,
            in_specs=[pl.BlockSpec(memory_space=pltpu.SMEM)] + [vmem] * 6,
            out_specs=(vmem, vmem, vmem),
            out_shape=(
                jax.ShapeDtypeStruct((M, W), BF16),
                jax.ShapeDtypeStruct((S // 2, W), BF16),
                jax.ShapeDtypeStruct((S // 2, W), BF16),
            ),
            scratch_shapes=[
                pltpu.VMEM((M, S), F32),
                pltpu.VMEM((M, 128), F32),
                pltpu.VMEM((R, S), F32),
                pltpu.VMEM((R, S), F32),
                pltpu.VMEM((M, S), BF16),
            ],
            compiler_params=pltpu.CompilerParams(vmem_limit_bytes=60 << 20),
            name="indexer",
        )(offs, packed, jnp.transpose(packed[:, :W]), hw, bias, kva, kvb)

        gkb = lax.ppermute(gkb, "core", [(0, 1), (1, 0)])
        gk = (gka.astype(F32) + gkb.astype(F32)).astype(BF16).reshape(xs * zs, rows, W)
        gk = lax.all_to_all(gk, "xz", split_axis=0, concat_axis=0, tiled=True)
        gk = jnp.sum(gk.astype(F32), axis=0).astype(BF16)
        last = jnp.concatenate(
            [gq.reshape(peers, M // peers, W), jnp.broadcast_to(gk[None], (peers, rows, W))], 1
        )
        last = lax.all_to_all(last, "head", split_axis=0, concat_axis=0, tiled=True)
        gq = last[:, : M // peers].reshape(peers, held, R, W)
        gq = jnp.transpose(gq, (0, 2, 1, 3)).reshape(rows, held, W).astype(F32)
        gk = jnp.sum(last[:, M // peers :].astype(F32), axis=0)
        return gq, gk

    return body


def solution(mesh):
    xs, zs, cores, zls, ys = 4, 4, 2, 2, 4
    grid = Mesh(mesh.devices.reshape(xs * zs, cores, zls * ys), ("xz", "core", "head"))
    ctx = ("xz", "core")
    return jax.shard_map(
        make_body(xs, zs, ys, zls),
        mesh=grid,
        in_specs=(
            P(ctx, "head", None),
            P(ctx, None),
            P(ctx, "head", None),
            P(ctx, None),
            P(ctx, "head"),
            P(),
        ),
        out_specs=(P(ctx, "head", None), P(ctx, None)),
        check_vma=False,
    )
```

```python
import math

import jax
import jax.numpy as jnp
from jax import lax
from jax.experimental import pallas as pl
from jax.experimental.pallas import tpu as pltpu
from jax.sharding import Mesh
from jax.sharding import PartitionSpec as P

SCALE_ATTN = 192.0 ** (-0.5)
LOG2E = math.log2(math.e)
LOSS_SCALE = 1024.0
NEGATIVE = -1e30
KEYS_STEP = 256
F32 = jnp.float32
BF16 = jnp.bfloat16


def nt(a, b):
    return lax.dot_general(a, b, (((1,), (1,)), ((), ())), preferred_element_type=F32)


def nn(a, b):
    return lax.dot_general(a, b, (((1,), (0,)), ((), ())), preferred_element_type=F32)


def kernel(offs_ref, p_ref, iqt_ref, hw_ref, bias_ref, kva_ref, kvb_ref, gq_ref, gka_ref, gkb_ref, s_ref, m_ref, x_ref, t_ref, c_ref, l_ref):
    M = p_ref.shape[0]
    R, S = bias_ref.shape
    W = iqt_ref.shape[0]
    heads = M // R
    step = KEYS_STEP
    lanes = step // 128
    tall = 32 * R
    half = kva_ref.shape[0]
    wide = kva_ref.shape[1]
    chunk = half // offs_ref.shape[0]
    qs = SCALE_ATTN * LOG2E

    m_ref[...] = jnp.full(m_ref.shape, NEGATIVE, F32)
    for part, kv_ref in enumerate((kva_ref, kvb_ref)):

        def fold(c, _):
            here = pl.multiple_of(c * step, step)
            base = pl.multiple_of(part * half + c * step, step)
            k = kv_ref[pl.ds(here, step), :W]
            bias = bias_ref[:, pl.ds(base, step)]
            total = jnp.zeros((R, step), F32)
            for g in range(0, M, tall):
                d = nt(p_ref[g : g + tall, :W], k)
                c_ref[g : g + tall, pl.ds(base, step)] = d.astype(BF16)
                for h in range(tall // R):
                    w = hw_ref[g + h * R : g + (h + 1) * R, :]
                    total = total + jnp.maximum(d[h * R : (h + 1) * R], 0.0) * jnp.concatenate([w] * lanes, 1)
            x_ref[:, pl.ds(base, step)] = total + bias
            lat = kv_ref[pl.ds(here, step), W:]
            for g in range(0, M, tall):
                d = nt(p_ref[g : g + tall, W:wide], lat)
                for h in range(tall // R):
                    rows = slice(g + h * R, g + (h + 1) * R)
                    s = d[h * R : (h + 1) * R] * qs + bias
                    s_ref[rows, pl.ds(base, step)] = s
                    top = m_ref[rows, :]
                    for l in range(lanes):
                        top = jnp.maximum(top, s[:, l * 128 : (l + 1) * 128])
                    m_ref[rows, :] = top
            return 0

        lax.fori_loop(0, half // step, fold, 0)

    m_ref[...] = jnp.broadcast_to(jnp.max(m_ref[...], axis=1, keepdims=True), m_ref.shape)

    def totals(g, _):
        rows = pl.ds(pl.multiple_of(g * 4 * R, 4 * R), 4 * R)
        top = m_ref[rows, :]
        acc = jnp.zeros((4 * R, 128), F32)
        for l in range(S // 128):
            acc = acc + jnp.exp2(s_ref[rows, l * 128 : (l + 1) * 128] - top)
        l_ref[rows, :] = acc
        return 0

    lax.fori_loop(0, heads // 4, totals, 0)
    m_ref[...] += jnp.broadcast_to(jnp.log2(jnp.sum(l_ref[...], axis=1, keepdims=True)), m_ref.shape)

    def targets(c, _):
        base = pl.multiple_of(c * step, step)
        acc = [jnp.zeros((R, 128), F32) for _ in range(lanes)]
        for h in range(heads):
            rows = slice(h * R, (h + 1) * R)
            m = m_ref[rows, :]
            for l in range(lanes):
                acc[l] = acc[l] + jnp.exp2(s_ref[rows, pl.ds(base + l * 128, 128)] - m)
        for l in range(lanes):
            t_ref[:, pl.ds(base + l * 128, 128)] = acc[l]
        return 0

    lax.fori_loop(0, S // step, targets, 0)

    x = x_ref[...]
    e = jnp.exp(x - jnp.max(x, axis=1, keepdims=True))
    prob = e * (1.0 / jnp.sum(e, axis=1, keepdims=True))
    delta = jnp.where(bias_ref[...] == 0.0, LOSS_SCALE * (prob - t_ref[...] * (1.0 / heads)), 0.0)
    t_ref[...] = delta.astype(BF16).astype(F32)

    def coefs(c, _):
        base = pl.multiple_of(c * step, step)
        delta = t_ref[:, pl.ds(base, step)]
        for h in range(heads):
            rows = slice(h * R, (h + 1) * R)
            w = hw_ref[rows, :]
            d = c_ref[rows, pl.ds(base, step)]
            value = (delta * jnp.concatenate([w] * lanes, 1)).astype(BF16)
            c_ref[rows, pl.ds(base, step)] = jnp.where(d > 0, value, jnp.zeros_like(value))
        return 0

    lax.fori_loop(0, S // step, coefs, 0)

    wide_step = 4 * step
    for part, gk_ref in enumerate((gka_ref, gkb_ref)):

        def keys(c, _):
            base = pl.multiple_of(part * half + c * wide_step, wide_step)
            gk = nn(iqt_ref[...], c_ref[:, pl.ds(base, wide_step)])
            gk = jnp.transpose(gk).astype(BF16)
            for e in range(wide_step // chunk):
                off = pl.multiple_of(offs_ref[c * (wide_step // chunk) + e], chunk)
                gk_ref[pl.ds(off, chunk), :] = gk[e * chunk : (e + 1) * chunk]
            return 0

        lax.fori_loop(0, half // wide_step, keys, 0)

    def index_queries(g, _):
        rows = pl.ds(pl.multiple_of(g * tall, tall), tall)
        gq = nn(c_ref[rows, :half], kva_ref[:, :W]) + nn(c_ref[rows, half:], kvb_ref[:, :W])
        gq_ref[rows, :] = gq.astype(BF16)
        return 0

    lax.fori_loop(0, M // tall, index_queries, 0)


def shifted(sizes, axis, by):
    total = sizes[0] * sizes[1]
    pairs = []
    for i in range(total):
        a, b = divmod(i, sizes[1])
        a, b = ((a + by) % sizes[0], b) if axis == 0 else (a, (b + by) % sizes[1])
        pairs.append((i, a * sizes[1] + b))
    return pairs


def make_body(xs, zs, ys, zls):
    def body(queries, latents, index_queries, index_keys, head_weights, block_pos):
        rows = queries.shape[0]
        peers = lax.axis_size("head")
        held = queries.shape[1]
        R = rows // peers
        M = R * held * peers
        W = index_queries.shape[2]
        quarter = rows // ys
        xz = lax.axis_index("xz")
        core = lax.axis_index("core")
        head = lax.axis_index("head")
        x, z, y = xz // zs, xz % zs, head % ys

        def along_x(a, by):
            return lax.ppermute(a, "xz", shifted((xs, zs), 0, by)) if by else a

        def along_z(a, by):
            return lax.ppermute(a, "xz", shifted((xs, zs), 1, by)) if by else a

        def along_y(a, by):
            return lax.ppermute(a, "head", shifted((zls, ys), 1, by)) if by else a

        width = W + latents.shape[1]
        spare = -width % 128
        own = jnp.concatenate([index_keys, latents, jnp.zeros((rows, spare), BF16)], 1)
        piece = lax.dynamic_slice_in_dim(own, y * quarter, quarter, 0)
        from_z = jnp.concatenate([along_z(piece, d) for d in range(1, zs)], 0)
        col = jnp.concatenate([along_x(piece, d) for d in range(xs)], 0)
        from_z, queries, index_queries = lax.optimization_barrier((from_z, queries, index_queries))
        hi = lax.reduce_precision(head_weights, 8, 7)
        rest = head_weights - hi
        mid = lax.reduce_precision(rest, 8, 7)
        pieces = jnp.stack([hi, mid, rest - mid], 2).astype(BF16)
        unused = jnp.zeros((rows, held, spare - 3), BF16)
        packed = jnp.concatenate([index_queries, queries, pieces, unused], 2)
        packed = jnp.transpose(packed.reshape(peers, R, held, -1), (0, 2, 1, 3))
        row = jnp.concatenate([along_y(from_z, d) for d in range(ys)], 0)
        row, packed = lax.optimization_barrier((row, packed))
        packed = lax.all_to_all(packed, "head", split_axis=0, concat_axis=0, tiled=True).reshape(M, -1)
        kva = [along_y(col, d) for d in range(ys)]
        for d in range(xs):
            kva.append(along_x(row, d))

        order = [(dx, 0, dy) for dy in range(ys) for dx in range(xs)]
        order += [(dx, dz, dy) for dx in range(xs) for dy in range(ys) for dz in range(1, zs)]
        order = jnp.array(order, jnp.int32)
        ox = (x - order[:, 0]) % xs
        oz = (z - order[:, 1]) % zs
        oy = (y - order[:, 2]) % ys
        offs = (ox * zs + oz) * rows + oy * quarter
        blocks = jnp.concatenate([(ox * zs + oz) * 2 + core, (ox * zs + oz) * 2 + 1 - core])
        ids = jnp.arange(block_pos.shape[0], dtype=jnp.int32)

        def place(block):
            return jnp.sum(jnp.where(block[:, None] == ids[None, :], block_pos[None, :], 0), axis=1) * rows

        key_pos = place(blocks) + jnp.concatenate([oy, oy]) * quarter
        key_pos = (key_pos[:, None] + jnp.arange(quarter, dtype=jnp.int32)[None, :]).reshape(-1)
        query_pos = place((xz * 2 + core)[None]) + head * R + jnp.arange(R, dtype=jnp.int32)
        bias = jnp.where(key_pos[None, :] <= query_pos[:, None], 0.0, NEGATIVE).astype(F32)
        S = key_pos.shape[0]

        hw = jnp.sum(packed[:, width : width + 3].astype(F32), axis=1, keepdims=True) * (W ** (-0.5))
        hw = jnp.broadcast_to(hw, (M, 128))
        iqt = jnp.transpose(packed[:, :W])
        kva = jnp.concatenate(kva, 0)
        kvb = lax.ppermute(kva, "core", [(0, 1), (1, 0)])

        vmem = pl.BlockSpec(memory_space=pltpu.VMEM)
        gq, gka, gkb = pl.pallas_call(
            kernel,
            in_specs=[pl.BlockSpec(memory_space=pltpu.SMEM)] + [vmem] * 6,
            out_specs=(vmem, vmem, vmem),
            out_shape=(
                jax.ShapeDtypeStruct((M, W), BF16),
                jax.ShapeDtypeStruct((S // 2, W), BF16),
                jax.ShapeDtypeStruct((S // 2, W), BF16),
            ),
            scratch_shapes=[
                pltpu.VMEM((M, S), F32),
                pltpu.VMEM((M, 128), F32),
                pltpu.VMEM((R, S), F32),
                pltpu.VMEM((R, S), F32),
                pltpu.VMEM((M, S), BF16),
                pltpu.VMEM((M, 128), F32),
            ],
            compiler_params=pltpu.CompilerParams(vmem_limit_bytes=60 << 20),
            name="indexer",
        )(offs, packed, iqt, hw, bias, kva, kvb)

        gkb = lax.ppermute(gkb, "core", [(0, 1), (1, 0)])
        gk = (gka.astype(F32) + gkb.astype(F32)).astype(BF16).reshape(xs * zs, rows, W)
        gk = lax.all_to_all(gk, "xz", split_axis=0, concat_axis=0, tiled=True)
        gk = jnp.sum(gk.astype(F32), axis=0).astype(BF16)
        last = jnp.concatenate(
            [gq.reshape(peers, M // peers, W), jnp.broadcast_to(gk[None], (peers, rows, W))], 1
        )
        last = lax.all_to_all(last, "head", split_axis=0, concat_axis=0, tiled=True)
        gq = last[:, : M // peers].reshape(peers, held, R, W)
        gq = jnp.transpose(gq, (0, 2, 1, 3)).reshape(rows, held, W).astype(F32)
        gk = jnp.sum(last[:, M // peers :].astype(F32), axis=0)
        return gq, gk

    return body


def solution(mesh):
    xs, zs, cores, zls, ys = 4, 4, 2, 2, 4
    grid = Mesh(mesh.devices.reshape(xs * zs, cores, zls * ys), ("xz", "core", "head"))
    ctx = ("xz", "core")
    return jax.shard_map(
        make_body(xs, zs, ys, zls),
        mesh=grid,
        in_specs=(
            P(ctx, "head", None),
            P(ctx, None),
            P(ctx, "head", None),
            P(ctx, None),
            P(ctx, "head"),
            P(),
        ),
        out_specs=(P(ctx, "head", None), P(ctx, None)),
        check_vma=False,
    )
```
